8 devices in a mesh: pz: 2 (over z, y), py: 4 (over x, core).
Axes of the slice: x: 2, y: 2, z: 1, core: 2. Of those that a mesh axis runs over, the one named last changes fastest.
Arguments:
- populations: float32 [19, 512, 32, 512], P(None, None, 'py', 'pz')
- relax_time: float32 [], replicated
- body_force: float32 [3], replicated
Outputs:
- output 1: float32 [19, 512, 32, 512], P(None, None, 'py', 'pz')
- output 2: float32 [512, 32, 512], P(None, 'py', 'pz')
- output 3: float32 [3, 512, 32, 512], P(None, None, 'py', 'pz')
All inputs are finite; a program needn't handle non-finite values.
Results may differ from the reference program's by a relative error of at most 0.001.
Values sent between devices are 32-bit elements.
A program may use at most 1 GiB of HBM per device.

```python
import jax
import jax.numpy as jnp

NX = 512
NY = 32
NZ = 512
SHARD_Y = 8
SHARD_Z = 256
STEPS = 4

VELOCITIES = ((0, 0, 0), (1, 0, 0), (-1, 0, 0), (0, 1, 0), (0, -1, 0), (0, 0, 1), (0, 0, -1), (1, 1, 0), (-1, -1, 0), (1, -1, 0), (-1, 1, 0), (1, 0, 1), (-1, 0, -1), (1, 0, -1), (-1, 0, 1), (0, 1, 1), (0, -1, -1), (0, 1, -1), (0, -1, 1))
WEIGHTS = (1.0 / 3.0,) + (1.0 / 18.0,) * 6 + (1.0 / 36.0,) * 12


def moments(populations, relax_time, body_force):
    density = jnp.sum(populations, axis=0)
    velocity = []
    for axis_id in range(3):
        plus_part = sum(populations[pop_id] for pop_id in range(19) if VELOCITIES[pop_id][axis_id] == 1)
        minus_part = sum(populations[pop_id] for pop_id in range(19) if VELOCITIES[pop_id][axis_id] == -1)
        velocity.append((plus_part - minus_part + body_force[axis_id] * relax_time) / density)
    return density, velocity


def equilibrium(density, velocity):
    speed_sq = velocity[0] * velocity[0] + velocity[1] * velocity[1] + velocity[2] * velocity[2]
    base_term = 1.0 - 1.5 * speed_sq
    result = []
    for pop_id in range(19):
        projection = sum(velocity[axis_id] * shift for axis_id, shift in enumerate(VELOCITIES[pop_id]) if shift != 0)
        result.append(WEIGHTS[pop_id] * density * (base_term + 3.0 * projection + 4.5 * projection * projection))
    return result


def collide(populations, relax_time, body_force):
    density, velocity = moments(populations, relax_time, body_force)
    feq_list = equilibrium(density, velocity)
    relax_rate = 1.0 / relax_time
    return [populations[pop_id] - (populations[pop_id] - feq_list[pop_id]) * relax_rate for pop_id in range(19)]


def propagate(collided):
    return jnp.stack([jnp.roll(collided[pop_id], VELOCITIES[pop_id], axis=(0, 1, 2)) for pop_id in range(19)])


def setup_inputs(seed: int = 0) -> dict:
    keys = jax.random.split(jax.random.key(seed), 7)
    grid_x = jnp.arange(NX, dtype=jnp.float32)[:, None, None]
    grid_y = jnp.arange(NY, dtype=jnp.float32)[None, :, None]
    grid_z = jnp.arange(NZ, dtype=jnp.float32)[None, None, :]
    phase = 2.0 * jnp.pi * jax.random.uniform(keys[0], (), jnp.float32)
    shear = 0.05 * jnp.sin(2.0 * jnp.pi * grid_z / NZ + phase)
    width_yz = max(2.0, 0.5 * min(SHARD_Y, SHARD_Z))
    width_x = max(2.0, NX / 8.0)
    dist_sq = ((grid_x - NX / 2.0) / width_x) ** 2 + ((grid_y - SHARD_Y + 0.5) / width_yz) ** 2 + ((grid_z - SHARD_Z + 0.5) / width_yz) ** 2
    pulse_amp = 0.1 + 0.1 * jax.random.uniform(keys[1], (), jnp.float32)
    density = 1.0 + pulse_amp * jnp.exp(-0.5 * dist_sq) + 0.02 * jax.random.normal(keys[2], (NX, NY, NZ), jnp.float32)
    noise_u = 0.01 * jax.random.normal(keys[3], (3, NX, NY, NZ), jnp.float32)
    velocity = [noise_u[0] + shear, noise_u[1], noise_u[2]]
    jitter = 1.0 + 0.1 * jax.random.normal(keys[4], (19, NX, NY, NZ), jnp.float32)
    populations = jnp.stack(equilibrium(density, velocity)) * jitter
    relax_time = 0.6 + 0.2 * jax.random.uniform(keys[5], (), jnp.float32)
    body_force = 0.004 * jax.random.normal(keys[6], (3,), jnp.float32)
    return {"populations": populations, "relax_time": relax_time, "body_force": body_force}


def reference(populations, relax_time, body_force):
    state = populations
    for step_id in range(STEPS):
        state = propagate(collide(state, relax_time, body_force))
    density, velocity = moments(state, relax_time, body_force)
    return state, density, jnp.stack(velocity)
```

```python
import functools

import jax
import jax.numpy as jnp
from jax import lax
from jax.experimental import pallas as pl
from jax.experimental.pallas import tpu as pltpu
from jax.sharding import PartitionSpec as P


MESH = pl.DeviceIdType.MESH
STEPS = 4
FORWARD = ((1, 0, 0), (0, 1, 0), (0, 0, 1), (1, 1, 0), (1, -1, 0), (1, 0, 1), (1, 0, -1), (0, 1, 1), (0, 1, -1))
VELOCITIES = ((0, 0, 0),) + tuple(tuple(sign * c for c in way) for way in FORWARD for sign in (1, -1))

STILL = tuple(p for p in range(19) if VELOCITIES[p][1] == 0)
UP = tuple(p for p in range(19) if VELOCITIES[p][1] == 1)
DOWN = tuple(p for p in range(19) if VELOCITIES[p][1] == -1)
ZPAIRS = tuple(
    (p, q) for p in range(19) for q in range(19)
    if VELOCITIES[p][2] == 1 and VELOCITIES[q] == VELOCITIES[p][:2] + (-1,))

C = 8
NS = 8
LAG = 3
RP = C * NS
LOOK = 2
NZ = 16
ZLAG = 6
PIECES = (10, 10, 12, 16, 16)
GROUP_ROWS = 2 * 5 * C * 2 + 8 + 2
Z_ROWS = 8 + 2
VMEM_BYTES = 62 * 2 ** 20


TILE = (8, 128)
GROUPS = (len(STILL), len(UP), len(DOWN))
F32 = jnp.float32


def splat(value):
    return jnp.full(TILE, value, F32)


def ring(pops, planes, *rows):
    return pltpu.VMEM((pops, planes, 2) + (rows or TILE[:1]) + TILE[1:], F32)


def sums(f, tau_g):
    s = {}
    d = {}
    for p in range(1, 19, 2):
        s[p] = f[p] + f[p + 1]
        d[p] = f[p] - f[p + 1]
    rho = f[0] + ((s[1] + s[3]) + (s[5] + s[7])) + ((s[9] + s[11]) + (s[13] + s[15])) + s[17]
    jx = (d[1] + (d[7] + d[9])) + ((d[11] + d[13]) + tau_g[0])
    jy = (d[3] + (d[7] - d[9])) + ((d[15] + d[17]) + tau_g[1])
    jz = (d[5] + (d[11] - d[13])) + ((d[15] - d[17]) + tau_g[2])
    return rho, (jx, jy, jz), s, d


def forced_moments(f, tau_g):
    rho, momentum, _, _ = sums(f, tau_g)
    inv = 1.0 / rho
    return rho, tuple(j * inv for j in momentum)


def collide(f, tau_g, rate36, keep, half_keep):
    rho, momentum, s, d = sums(f, tau_g)
    inv3 = 3.0 / rho
    u3 = tuple(j * inv3 for j in momentum)
    rw = rate36 * rho
    odd = tuple(rw * u for u in u3)
    square = tuple(u * o for u, o in zip(u3, odd))
    pair_square = {(0, 1): square[0] + square[1], (0, 2): square[0] + square[2], (1, 2): square[1] + square[2]}
    even = rw - (pair_square[0, 1] + square[2]) * (1.0 / 6.0)
    even2 = even + even
    out = [None] * 19
    out[0] = keep * f[0] + 12.0 * even

    def relax(p, e, o):
        e = half_keep * s[p] + e
        o = half_keep * d[p] + o
        out[p] = e + o
        out[p + 1] = e - o

    for axis in range(3):
        relax(2 * axis + 1, even2 + square[axis], odd[axis] + odd[axis])
    for p, (a, b) in ((7, (0, 1)), (11, (0, 2)), (15, (1, 2))):
        mean = even + 0.5 * pair_square[a, b]
        cross = u3[a] * odd[b]
        relax(p, mean + cross, odd[a] + odd[b])
        relax(p + 2, mean - cross, odd[a] - odd[b])
    return out


def pull(still, up, down, zhalo, planes, lanes):
    halves = ([None] * 19, [None] * 19)
    edges = {}
    for p in range(19):
        cx, cy, cz = VELOCITIES[p]
        plane, place = planes[cx]
        if cy == 0:
            lo, hi = (still[STILL.index(p), plane, h] for h in range(2))
        elif cy == 1:
            lo, hi = (up[UP.index(p), plane, h, 7:15, :] for h in range(2))
        else:
            lo, hi = (down[DOWN.index(p), plane, h, 1:9, :] for h in range(2))
        if cz != 0:
            if p in edges:
                edge = edges[p]
            else:
                pair = next(n for n, pops in enumerate(ZPAIRS) if p in pops)
                edge = turn(zhalo(cx, slice(8 - cy, 16 - cy)), 127 - 2 * (pair * C + place))
                edges.update((pop, edge) for pop in ZPAIRS[pair])
            if cz == 1:
                lo = jnp.where(lanes == 0, edge, lo)
            else:
                hi = jnp.where(lanes == 127, edge, hi)
        halves[0][p] = lo
        halves[1][p] = hi
    return halves


def turn(value, amount):
    return pltpu.roll(value, amount, 1) if amount % 128 else value


def push(halves, lanes):
    column = None
    for n, (p, q) in enumerate(ZPAIRS):
        lo, hi = turn(halves[0][p], 1), turn(halves[1][p], 1)
        halves[0][p], halves[1][p] = lo, jnp.where(lanes == 0, lo, hi)
        back_lo, back_hi = turn(halves[0][q], 127), turn(halves[1][q], 127)
        halves[0][q], halves[1][q] = jnp.where(lanes == 127, back_hi, back_lo), back_hi
        leaving = turn(jnp.where(lanes == 0, hi, back_lo), 2 * n * C + 1)
        column = leaving if column is None else jnp.where(lanes >= 2 * n * C, leaving, column)
    return column


def march_kernel(
    chunks, tau_ref, force_ref, pops, *refs,
):
    g_still, g_up, g_down, z_halo = refs[:4]
    faces = refs[4:4 + 2 * len(PIECES)]
    (buf_in, rings, out_still, out_up, out_down, out_z, in_z,
    in_sem, out_sem, face_sem, send_sem, recv_sem, zsend_sem, zrecv_sem, ysend_sem, yrecv_sem, tally,
    ) = refs[4 + 2 * len(PIECES):]
    still, up, down, zsend, zrecv = rings
    py, pz = lax.axis_index("py"), lax.axis_index("pz")
    py_up, py_down, pz_other = lax.rem(py + 1, 4), lax.rem(py + 3, 4), 1 - pz
    above = {"py": py_up, "pz": pz}
    below = {"py": py_down, "pz": pz}
    beside = {"py": py, "pz": pz_other}
    corner_above = {"py": py_up, "pz": pz_other}
    corner_below = {"py": py_down, "pz": pz_other}
    in_z[...] = jnp.zeros_like(in_z)
    barrier = pltpu.get_barrier_semaphore()
    for peer in (above, below, beside, corner_above, corner_below):
        pl.semaphore_signal(barrier, inc=1, device_id=peer, device_id_type=MESH)

    def load(k, slot):
        return pltpu.make_async_copy(
            pops.at[:, pl.ds(lax.rem(k, chunks) * C, C)], buf_in.at[slot], in_sem.at[slot])

    load(0, 0).start()
    load(1, 1).start()

    tau = splat(tau_ref[0])
    rate = 1.0 / tau
    keep = 1.0 - rate
    half_keep = 0.5 * keep
    rate36 = rate * (1.0 / 36.0)
    tau_g = tuple(tau * force_ref[axis] for axis in range(3))
    lanes = lax.broadcasted_iota(jnp.int32, TILE, 1)
    places = lanes & (2 * C - 1)

    def sends(s, slot):
        rows = pl.ds(slot * C, C)
        pairs = (
            (up[s].at[:, rows, :, 15], up[s].at[:, rows, :, 7], above),
            (down[s].at[:, rows, :, 0], down[s].at[:, rows, :, 8], below),
            (zsend[s].at[slot], zrecv[s].at[slot, 8:16], beside),
            (zsend[s].at[slot, 7:8], zrecv[s].at[slot, 7:8], corner_above),
            (zsend[s].at[slot, 0:1], zrecv[s].at[slot, 16:17], corner_below),
        )
        return [
            pltpu.make_async_remote_copy(
                src_ref=src, dst_ref=dst, send_sem=send_sem.at[s, slot], recv_sem=recv_sem.at[s, slot],
                device_id=peer, device_id_type=MESH)
            for src, dst, peer in pairs
        ]

    def settle(sem, rows):
        pltpu.make_async_copy(tally.at[:rows], tally.at[:rows], sem).wait()

    def writes(k, slot):
        rows = pl.ds(k * C, C)
        pairs = (
            (out_still.at[slot], g_still.at[:, rows]),
            (out_up.at[slot], g_up.at[:, rows]),
            (out_down.at[slot], g_down.at[:, rows]),
        )
        return [pltpu.make_async_copy(src, dst, out_sem.at[slot, n]) for n, (src, dst) in enumerate(pairs)]

    def face_moves(k, act, pieces=len(PIECES)):
        slot = lax.rem(k, 2)
        for n, low, high, base in face_spans(chunks):
            if n >= pieces:
                continue

            def move(n=n, base=base):
                rows = pl.ds((k - base) * C, C)
                pairs = (
                    (out_up.at[slot, :, :, :, 7], faces[2 * n].at[:, rows], above),
                    (out_down.at[slot, :, :, :, 0], faces[2 * n + 1].at[:, rows], below),
                )
                for m, (face, dst, peer) in enumerate(pairs):
                    if n:
                        act(pltpu.make_async_copy(face, dst, face_sem.at[slot, n % 2, m]), False)
                    else:
                        act(pltpu.make_async_remote_copy(
                            src_ref=face, dst_ref=dst, send_sem=ysend_sem.at[slot, m], recv_sem=yrecv_sem.at[k, m],
                            device_id=peer, device_id_type=MESH), True)

            pl.when((k >= low) & (k < high))(move)

    def face_reclaim(k):
        face_moves(k, lambda copy, remote: copy.wait_send() if remote else copy.wait())

    def z_sends(k):
        slot = lax.rem(k, NZ)
        pairs = (
            (out_z.at[slot], in_z.at[k, 8:16], beside),
            (out_z.at[slot, 7:8], in_z.at[k, 7:8], corner_above),
            (out_z.at[slot, 0:1], in_z.at[k, 16:17], corner_below),
        )
        return [
            pltpu.make_async_remote_copy(
                src_ref=src, dst_ref=dst, send_sem=zsend_sem.at[slot], recv_sem=zrecv_sem.at[slot],
                device_id=peer, device_id_type=MESH)
            for src, dst, peer in pairs
        ]

    def fetch(s, k, j):
        slot = lax.rem(k, NS)
        if s == 0:
            return [
                [buf_in[lax.rem(k, 2), p, j, :, 128 * h:128 * h + 128] for p in range(19)] for h in range(2)]
        planes = {}
        slots = {}
        for cx in (1, 0, -1):
            ahead, place = divmod(j + 1 - cx, C)
            slots[cx] = slot if ahead == 0 else lax.rem(k + 1, NS)
            planes[cx] = (slots[cx] * C + place, place)
        zhalo = lambda cx, rows: zrecv[s - 1][slots[cx], rows, :]
        return pull(still[s - 1], up[s - 1], down[s - 1], zhalo, planes, lanes)

    def keep_plane(s, k, j, halves):
        at = lax.rem(k, NS) * C + j
        out_slot = lax.rem(k, 2)
        for h in range(2):
            for p in range(19):
                cy = VELOCITIES[p][1]
                if s < 3:
                    if cy == 0:
                        still[s][STILL.index(p), at, h] = halves[h][p]
                    elif cy == 1:
                        up[s][UP.index(p), at, h, 8:16, :] = halves[h][p]
                    else:
                        down[s][DOWN.index(p), at, h, 0:8, :] = halves[h][p]
                elif cy == 0:
                    out_still[out_slot, STILL.index(p), j, h] = halves[h][p]
                elif cy == 1:
                    out_up[out_slot, UP.index(p), j, h] = halves[h][p]
                else:
                    out_down[out_slot, DOWN.index(p), j, h] = halves[h][p]

    def compute(work):
        tasks = [(s, k, j) for s, k in work for j in range(C)]
        fetched = []
        packed = None
        for n, (s, k, j) in enumerate(tasks):
            while len(fetched) < min(n + LOOK + 1, len(tasks)):
                fetched.append(fetch(*tasks[len(fetched)]))
            halves = [collide(fetched[n][h], tau_g, rate36, keep, half_keep) for h in range(2)]
            column = turn(push(halves, lanes), 2 * j)
            packed = column if j == 0 else jnp.where(places >= 2 * j, column, packed)
            keep_plane(s, k, j, halves)
            if j == C - 1:
                if s < 3:
                    zsend[s][lax.rem(k, NS)] = packed
                else:
                    out_z[lax.rem(k, NZ)] = packed
                send(s, k)

    def send(s, k):
        if s < 3:
            for copy in sends(s, lax.rem(k, NS)):
                copy.start()
        else:
            for copy in writes(k, lax.rem(k, 2)) + z_sends(k):
                copy.start()
            face_moves(k, lambda copy, remote: copy.start())

    def arrive(s, k):
        if s == 0:
            load(k, lax.rem(k, 2)).wait()
        else:
            settle(recv_sem.at[s - 1, lax.rem(k + 1, NS)], GROUP_ROWS)

    def reclaim(s, k):
        if s < 3:
            settle(send_sem.at[s, lax.rem(k, NS)], GROUP_ROWS)
        else:
            for copy in writes(k - 2, lax.rem(k, 2)):
                copy.wait()
            face_reclaim(k - 2)

    def stage(s, i):
        k = i - s * LAG
        last = chunks if s < 3 else chunks - 1

        @pl.when((k >= 0) & (k <= last))
        def _():
            if s > 0:
                @pl.when(k == 0)
                def _():
                    arrive(s, -1)
            pl.when(k < chunks + (s == 0))(lambda: arrive(s, k))
            pl.when(k >= (NS if s < 3 else 2))(lambda: reclaim(s, k))
            if s == 0:
                pl.when(k == 0)(lambda: pl.semaphore_wait(barrier, 5))
            if s == 3:
                pl.when(k >= NZ)(lambda: settle(zsend_sem.at[lax.rem(k, NZ)], Z_ROWS))
                pl.when(k >= ZLAG)(lambda: settle(zrecv_sem.at[lax.rem(k - ZLAG, NZ)], Z_ROWS))
            compute([(s, k)])
            if s == 0:
                pl.when(k + 2 <= chunks)(lambda: load(k + 2, lax.rem(k, 2)).start())

    def step(i, carry):
        for s in range(STEPS):
            stage(s, i)
        return carry

    lax.fori_loop(0, chunks + 3 * LAG, step, 0)

    def repeat(low, high, wait):
        def one(n, carry):
            wait(n)
            return carry

        lax.fori_loop(low, high, one, 0)

    for s in range(STEPS - 1):
        repeat(0, NS, lambda slot: settle(send_sem.at[s, slot], GROUP_ROWS))
    repeat(chunks - ZLAG, chunks, lambda k: settle(zrecv_sem.at[lax.rem(k, NZ)], Z_ROWS))
    last = pltpu.make_async_copy(in_z, z_halo, in_sem.at[0])
    last.start()
    repeat(0, NZ, lambda slot: settle(zsend_sem.at[slot], Z_ROWS))
    for k in (chunks - 2, chunks - 1):
        for copy in writes(k, k % 2):
            copy.wait()
        face_reclaim(k)

    def face_arrive(k):
        face_moves(k, lambda copy, remote: copy.wait_recv(), 1)

    repeat(0, PIECES[0] + 1, face_arrive)
    last.wait()


def face_spans(chunks):
    spans = []
    base = 0
    for n, count in enumerate(PIECES):
        high = base + count + 1
        spans.append((n, base, min(high, chunks), base))
        if high > chunks:
            spans.append((n, 0, high - chunks, base - chunks))
        base += count
    return spans


def march(relax_time, body_force, populations):
    nx = populations.shape[1]
    chunks = nx // C
    state = [jax.ShapeDtypeStruct((pops, nx, 2) + TILE, F32) for pops in GROUPS]
    halo_z = (chunks, 3 * TILE[0], TILE[1])
    faces = [
        jax.ShapeDtypeStruct((pops, (count + 1) * C, 2, TILE[1]), F32) for count in PIECES for pops in GROUPS[1:]]
    anywhere = pl.BlockSpec(memory_space=pl.ANY)
    outs = state + [jax.ShapeDtypeStruct(halo_z, F32)] + faces
    dma = pltpu.SemaphoreType.DMA
    stages = STEPS - 1
    wide = 2 * TILE[0]
    return pl.pallas_call(
        functools.partial(march_kernel, chunks),
        out_shape=outs,
        in_specs=[pl.BlockSpec(memory_space=pltpu.SMEM)] * 2 + [anywhere],
        out_specs=[anywhere] * len(outs),
        scratch_shapes=[
            pltpu.VMEM((2, populations.shape[0], C) + populations.shape[2:], F32),
            [
                [ring(GROUPS[0], RP)] * stages, [ring(GROUPS[1], RP, wide)] * stages, [ring(GROUPS[2], RP, wide)] * stages,
                [pltpu.VMEM((NS,) + TILE, F32)] * stages, [pltpu.VMEM((NS,) + halo_z[1:], F32)] * stages,
            ],
            *[pltpu.VMEM((2, pops, C, 2) + TILE, F32) for pops in GROUPS],
            pltpu.VMEM((NZ,) + TILE, F32), pltpu.VMEM(halo_z, F32),
            dma((2,)), dma((2, 3)), dma((2, 2, 2)), dma((stages, NS)), dma((stages, NS)), dma((NZ,)), dma((NZ,)),
            dma((2, 2)), dma((PIECES[0] + 1, 2)),
            pltpu.VMEM((GROUP_ROWS, TILE[1]), F32),
        ],
        compiler_params=pltpu.CompilerParams(collective_id=0, has_side_effects=True, vmem_limit_bytes=VMEM_BYTES),
        cost_estimate=pl.CostEstimate(flops=10 ** 9, bytes_accessed=10 ** 8, transcendentals=0),
        name="march",
    )(relax_time, body_force, populations)


KW = 3
KR = 4


def final_kernel(
    first, count, aliased, tau_ref, force_ref, g_still, g_up, g_down, halo_up, halo_down, z_in, *rest,
):
    rest = rest[3:] if aliased else rest
    pops, density, velocity, still, up, down, zs, out_f, out_m, in_sem, out_sem, z_sem = rest
    chunks = g_still.shape[1] // C
    tau = splat(tau_ref[0])
    tau_g = tuple(tau * force_ref[axis] for axis in range(3))
    lanes = lax.broadcasted_iota(jnp.int32, TILE, 1)

    z_copy = pltpu.make_async_copy(z_in, zs, z_sem)
    z_copy.start()

    def state_loads(t):
        slot = lax.rem(t, KR)
        src = pl.ds(lax.rem(first + t + chunks - 1, chunks) * C, C)
        dst = pl.ds(slot * C, C)
        return [
            pltpu.make_async_copy(g_still.at[:, src], still.at[:, dst], in_sem.at[slot, 0]),
            pltpu.make_async_copy(g_up.at[:, src], up.at[:, dst, :, 8:16], in_sem.at[slot, 1]),
            pltpu.make_async_copy(g_down.at[:, src], down.at[:, dst, :, 0:8], in_sem.at[slot, 2]),
        ]

    def halo_loads(t, skip, size):
        slot = lax.rem(t, KR)
        src = pl.ds(t * C + skip, size)
        dst = pl.ds(slot * C + skip, size)
        return [
            pltpu.make_async_copy(halo_up.at[:, src], up.at[:, dst, :, 7], in_sem.at[slot, 3]),
            pltpu.make_async_copy(halo_down.at[:, src], down.at[:, dst, :, 8], in_sem.at[slot, 4]),
        ]

    def loads(t, act):
        for copy in state_loads(t):
            act(copy)
        for cond, skip, size in ((t == 0, 4, 4), ((t > 0) & (t < count), 0, C), (t == count, 0, 6)):
            @pl.when(cond)
            def _():
                for copy in halo_loads(t, skip, size):
                    act(copy)

    def writes(t):
        slot = lax.rem(t, KW)
        dst = pl.ds(lax.rem(first + t - 1, chunks) * C, C)
        return [
            pltpu.make_async_copy(out_f.at[slot], pops.at[:, dst], out_sem.at[slot, 0]),
            pltpu.make_async_copy(out_m.at[slot, 0], density.at[dst], out_sem.at[slot, 1]),
            pltpu.make_async_copy(out_m.at[slot, pl.ds(1, 3)], velocity.at[:, dst], out_sem.at[slot, 2]),
        ]

    start = lambda copy: copy.start()
    finish = lambda copy: copy.wait()
    for t in range(3):
        loads(t, start)
    loads(0, finish)
    z_copy.wait()

    def step(t, carry):
        @pl.when(t + 2 <= count)
        def _():
            loads(t + 2, start)

        loads(t, finish)

        @pl.when(t > KW)
        def _():
            for copy in writes(t - KW):
                copy.wait()

        slot = lax.rem(t, KW)

        for j in range(C):
            planes = {}
            chunk = {}
            for cx in (1, 0, -1):
                ahead, place = divmod(5 + j - cx, C)
                planes[cx] = (lax.rem(t - 1 + ahead, KR) * C + place, place)
                chunk[cx] = lax.rem(first - 2 + ahead + t + chunks, chunks)
            zhalo = lambda cx, rows: zs[chunk[cx], rows, :]
            halves = pull(still, up, down, zhalo, planes, lanes)
            for h in range(2):
                f = halves[h]
                rho, u = forced_moments(f, tau_g)
                window = slice(128 * h, 128 * h + 128)
                for p in range(19):
                    out_f[slot, p, j, :, window] = f[p]
                for n, value in enumerate((rho,) + u):
                    out_m[slot, n, j, :, window] = value
        for copy in writes(t):
            copy.start()
        return carry

    lax.fori_loop(1, count + 1, step, 0)
    for t in range(count + 1 - KW, count + 1):
        for copy in writes(t):
            copy.wait()


def final(first, count, relax_time, body_force, state, halos, outs):
    nx = state[0].shape[1]
    chunks = nx // C
    anywhere = pl.BlockSpec(memory_space=pl.ANY)
    aliased = outs is not None
    operands = (relax_time, body_force) + state + halos + (outs if aliased else ())
    base = len(operands) - 3
    block = (TILE[0], 2 * TILE[1])
    dma = pltpu.SemaphoreType.DMA
    wide = 2 * TILE[0]
    return pl.pallas_call(
        functools.partial(final_kernel, first, count, aliased),
        out_shape=tuple(jax.ShapeDtypeStruct(lead + (nx,) + block, F32) for lead in ((sum(GROUPS),), (), (3,))),
        in_specs=[pl.BlockSpec(memory_space=pltpu.SMEM)] * 2 + [anywhere] * (len(operands) - 2),
        out_specs=(anywhere,) * 3,
        input_output_aliases={base + n: n for n in range(3)} if aliased else {},
        scratch_shapes=[
            ring(GROUPS[0], KR * C), ring(GROUPS[1], KR * C, wide), ring(GROUPS[2], KR * C, wide),
            pltpu.VMEM((chunks, 3 * TILE[0], TILE[1]), F32),
            pltpu.VMEM((KW, sum(GROUPS), C) + block, F32), pltpu.VMEM((KW, 4, C) + block, F32),
            dma((KR, 5)), dma((KW, 3)), dma,
        ],
        compiler_params=pltpu.CompilerParams(vmem_limit_bytes=48 * 2 ** 20),
        cost_estimate=pl.CostEstimate(flops=count * 10 ** 6, bytes_accessed=count * 3 * 10 ** 6, transcendentals=0),
        name="final",
    )(*operands)


def solution(mesh):
    size_y = mesh.shape["py"]
    size_z = mesh.shape["pz"]
    field_spec = P(None, None, "py", "pz")

    def shift(block, dy, dz):
        pairs = []
        for z in range(size_z):
            for y in range(size_y):
                pairs.append((z * size_y + y, (z + dz) % size_z * size_y + (y + dy) % size_y))
        return lax.ppermute(block, ("pz", "py"), pairs)

    def local_steps(populations, relax_time, body_force):
        tau = relax_time.reshape((1,))
        *state, z_halo = (marched := march(tau, body_force, populations))[:4]
        faces = marched[4:]
        outs = None
        first = 1
        for n, count in enumerate(PIECES):
            up, down = faces[2 * n:2 * n + 2]
            if n:
                up = shift(up, 1, 0)
                down = shift(down, -1, 0)
            outs = final(first, count, tau, body_force, tuple(state), (up, down, z_halo), outs)
            first += count
        return tuple(outs)

    return jax.shard_map(local_steps, mesh=mesh, in_specs=(field_spec, P(), P()), out_specs=(field_spec, P(None, "py", "pz"), field_spec), check_vma=False)
```

```python
import functools

import jax
import jax.numpy as jnp
from jax import lax
from jax.experimental import pallas as pl
from jax.experimental.pallas import tpu as pltpu
from jax.sharding import PartitionSpec as P


MESH = pl.DeviceIdType.MESH
STEPS = 4
FORWARD = ((1, 0, 0), (0, 1, 0), (0, 0, 1), (1, 1, 0), (1, -1, 0), (1, 0, 1), (1, 0, -1), (0, 1, 1), (0, 1, -1))
VELOCITIES = ((0, 0, 0),) + tuple(tuple(sign * c for c in way) for way in FORWARD for sign in (1, -1))

STILL = tuple(p for p in range(19) if VELOCITIES[p][1] == 0)
UP = tuple(p for p in range(19) if VELOCITIES[p][1] == 1)
DOWN = tuple(p for p in range(19) if VELOCITIES[p][1] == -1)
ZPAIRS = tuple(
    (p, q) for p in range(19) for q in range(19)
    if VELOCITIES[p][2] == 1 and VELOCITIES[q] == VELOCITIES[p][:2] + (-1,))

C = 8
NS = 9
LAG = 4
RP = C * NS
LOOK = 2
NZ = 16
ZLAG = 8
PIECES = (16, 20, 28)
GROUP_ROWS = 2 * 5 * C * 2 + 8 + 2
Z_ROWS = 8 + 2
VMEM_BYTES = 62 * 2 ** 20


TILE = (8, 128)
GROUPS = (len(STILL), len(UP), len(DOWN))
F32 = jnp.float32


def splat(value):
    return jnp.full(TILE, value, F32)


def ring(pops, planes, rows=8):
    return pltpu.VMEM((span(pops, planes), rows) + TILE[1:], F32)


def span(pops, planes=C):
    return planes * pops * 2


def cell(group, p, slot, place, half):
    return slot * span(len(group)) + (place * len(group) + group.index(p)) * 2 + half


def sums(f, tau_g):
    s = {}
    d = {}
    for p in range(1, 19, 2):
        s[p] = f[p] + f[p + 1]
        d[p] = f[p] - f[p + 1]
    rho = f[0] + ((s[1] + s[3]) + (s[5] + s[7])) + ((s[9] + s[11]) + (s[13] + s[15])) + s[17]
    jx = (d[1] + (d[7] + d[9])) + ((d[11] + d[13]) + tau_g[0])
    jy = (d[3] + (d[7] - d[9])) + ((d[15] + d[17]) + tau_g[1])
    jz = (d[5] + (d[11] - d[13])) + ((d[15] - d[17]) + tau_g[2])
    return rho, (jx, jy, jz), s, d


def forced_moments(f, tau_g):
    rho, momentum, _, _ = sums(f, tau_g)
    inv = 1.0 / rho
    return rho, tuple(j * inv for j in momentum)


def collide(f, tau_g, rate36, keep, half_keep):
    rho, momentum, s, d = sums(f, tau_g)
    inv3 = 3.0 / rho
    u3 = tuple(j * inv3 for j in momentum)
    rw = rate36 * rho
    odd = tuple(rw * u for u in u3)
    square = tuple(u * o for u, o in zip(u3, odd))
    pair_square = {(0, 1): square[0] + square[1], (0, 2): square[0] + square[2], (1, 2): square[1] + square[2]}
    even = rw - (pair_square[0, 1] + square[2]) * (1.0 / 6.0)
    even2 = even + even
    out = [None] * 19
    out[0] = keep * f[0] + 12.0 * even

    def relax(p, e, o):
        e = half_keep * s[p] + e
        o = half_keep * d[p] + o
        out[p] = e + o
        out[p + 1] = e - o

    for axis in range(3):
        relax(2 * axis + 1, even2 + square[axis], odd[axis] + odd[axis])
    for p, (a, b) in ((7, (0, 1)), (11, (0, 2)), (15, (1, 2))):
        mean = even + 0.5 * pair_square[a, b]
        cross = u3[a] * odd[b]
        relax(p, mean + cross, odd[a] + odd[b])
        relax(p + 2, mean - cross, odd[a] - odd[b])
    return out


def pull(still, up, down, zhalo, planes, lanes):
    halves = ([None] * 19, [None] * 19)
    edges = {}
    for p in range(19):
        cx, cy, cz = VELOCITIES[p]
        slot, place = planes[cx]
        if cy == 0:
            lo, hi = (still[cell(STILL, p, slot, place, h)] for h in range(2))
        elif cy == 1:
            lo, hi = (up[cell(UP, p, slot, place, h), 7:15, :] for h in range(2))
        else:
            lo, hi = (down[cell(DOWN, p, slot, place, h), 1:9, :] for h in range(2))
        if cz != 0:
            if p in edges:
                edge = edges[p]
            else:
                pair = next(n for n, pops in enumerate(ZPAIRS) if p in pops)
                edge = turn(zhalo(cx, slice(8 - cy, 16 - cy)), 127 - 2 * (pair * C + place))
                edges.update((pop, edge) for pop in ZPAIRS[pair])
            if cz == 1:
                lo = jnp.where(lanes == 0, edge, lo)
            else:
                hi = jnp.where(lanes == 127, edge, hi)
        halves[0][p] = lo
        halves[1][p] = hi
    return halves


def turn(value, amount):
    return pltpu.roll(value, amount, 1) if amount % 128 else value


def push(halves, lanes):
    column = None
    for n, (p, q) in enumerate(ZPAIRS):
        lo, hi = turn(halves[0][p], 1), turn(halves[1][p], 1)
        halves[0][p], halves[1][p] = lo, jnp.where(lanes == 0, lo, hi)
        back_lo, back_hi = turn(halves[0][q], 127), turn(halves[1][q], 127)
        halves[0][q], halves[1][q] = jnp.where(lanes == 127, back_hi, back_lo), back_hi
        leaving = turn(jnp.where(lanes == 0, hi, back_lo), 2 * n * C + 1)
        column = leaving if column is None else jnp.where(lanes >= 2 * n * C, leaving, column)
    return column


def march_kernel(
    chunks, tau_ref, force_ref, pops, *refs,
):
    g_still, g_up, g_down, z_halo = refs[:4]
    faces = refs[4:4 + 2 * len(PIECES)]
    (buf_in, rings, out_still, out_up, out_down, out_z, in_z,
    in_sem, out_sem, face_sem, send_sem, recv_sem, zsend_sem, zrecv_sem, ysend_sem, yrecv_sem, tally,
    ) = refs[4 + 2 * len(PIECES):]
    still, up, down, zsend, zrecv = rings
    py, pz = lax.axis_index("py"), lax.axis_index("pz")
    py_up, py_down, pz_other = lax.rem(py + 1, 4), lax.rem(py + 3, 4), 1 - pz
    above = {"py": py_up, "pz": pz}
    below = {"py": py_down, "pz": pz}
    beside = {"py": py, "pz": pz_other}
    corner_above = {"py": py_up, "pz": pz_other}
    corner_below = {"py": py_down, "pz": pz_other}
    in_z[...] = jnp.zeros_like(in_z)
    barrier = pltpu.get_barrier_semaphore()
    for peer in (above, below, beside, corner_above, corner_below):
        pl.semaphore_signal(barrier, inc=1, device_id=peer, device_id_type=MESH)

    def load(k, slot):
        return pltpu.make_async_copy(
            pops.at[:, pl.ds(lax.rem(k, chunks) * C, C)], buf_in.at[slot], in_sem.at[slot])

    load(0, 0).start()
    load(1, 1).start()

    tau = splat(tau_ref[0])
    rate = 1.0 / tau
    keep = 1.0 - rate
    half_keep = 0.5 * keep
    rate36 = rate * (1.0 / 36.0)
    tau_g = tuple(tau * force_ref[axis] for axis in range(3))
    lanes = lax.broadcasted_iota(jnp.int32, TILE, 1)
    places = lanes & (2 * C - 1)

    def sends(s, slot):
        rows = pl.ds(slot * span(5), span(5))
        pairs = (
            (up[s].at[rows, 15], up[s].at[rows, 7], above),
            (down[s].at[rows, 0], down[s].at[rows, 8], below),
            (zsend[s].at[slot], zrecv[s].at[slot, 8:16], beside),
            (zsend[s].at[slot, 7:8], zrecv[s].at[slot, 7:8], corner_above),
            (zsend[s].at[slot, 0:1], zrecv[s].at[slot, 16:17], corner_below),
        )
        return [
            pltpu.make_async_remote_copy(
                src_ref=src, dst_ref=dst, send_sem=send_sem.at[s, slot], recv_sem=recv_sem.at[s, slot],
                device_id=peer, device_id_type=MESH)
            for src, dst, peer in pairs
        ]

    def settle(sem, rows):
        pltpu.make_async_copy(tally.at[:rows], tally.at[:rows], sem).wait()

    def writes(k, slot):
        pairs = [
            (out.at[slot], state.at[pl.ds(k * span(pops), span(pops))])
            for pops, out, state in zip(GROUPS, (out_still, out_up, out_down), (g_still, g_up, g_down))]
        return [pltpu.make_async_copy(src, dst, out_sem.at[slot, n]) for n, (src, dst) in enumerate(pairs)]

    def face_moves(k, act, pieces=len(PIECES)):
        slot = lax.rem(k, 2)
        for n, low, high, base in face_spans(chunks):
            if n >= pieces:
                continue

            def move(n=n, base=base):
                rows = pl.ds((k - base) * span(5), span(5))
                pairs = (
                    (out_up.at[slot, :, 7], faces[2 * n].at[rows], above),
                    (out_down.at[slot, :, 0], faces[2 * n + 1].at[rows], below),
                )
                for m, (face, dst, peer) in enumerate(pairs):
                    if n:
                        act(pltpu.make_async_copy(face, dst, face_sem.at[slot, n % 2, m]), False)
                    else:
                        act(pltpu.make_async_remote_copy(
                            src_ref=face, dst_ref=dst, send_sem=ysend_sem.at[slot, m], recv_sem=yrecv_sem.at[k, m],
                            device_id=peer, device_id_type=MESH), True)

            pl.when((k >= low) & (k < high))(move)

    def face_reclaim(k):
        face_moves(k, lambda copy, remote: copy.wait_send() if remote else copy.wait())

    def z_sends(k):
        slot = lax.rem(k, NZ)
        pairs = (
            (out_z.at[slot], in_z.at[k, 8:16], beside),
            (out_z.at[slot, 7:8], in_z.at[k, 7:8], corner_above),
            (out_z.at[slot, 0:1], in_z.at[k, 16:17], corner_below),
        )
        return [
            pltpu.make_async_remote_copy(
                src_ref=src, dst_ref=dst, send_sem=zsend_sem.at[slot], recv_sem=zrecv_sem.at[slot],
                device_id=peer, device_id_type=MESH)
            for src, dst, peer in pairs
        ]

    def fetch(s, k, j):
        slot = lax.rem(k, NS)
        if s == 0:
            return [
                [buf_in[lax.rem(k, 2), p, j, :, 128 * h:128 * h + 128] for p in range(19)] for h in range(2)]
        planes = {}
        slots = {}
        for cx in (1, 0, -1):
            ahead, place = divmod(j + 1 - cx, C)
            slots[cx] = slot if ahead == 0 else lax.rem(k + 1, NS)
            planes[cx] = (slots[cx], place)
        zhalo = lambda cx, rows: zrecv[s - 1][slots[cx], rows, :]
        return pull(still[s - 1], up[s - 1], down[s - 1], zhalo, planes, lanes)

    def keep_plane(s, k, j, halves):
        at = lax.rem(k, NS)
        out_slot = lax.rem(k, 2)
        for group, kept, out, row in ((STILL, still, out_still, 0), (UP, up, out_up, 8), (DOWN, down, out_down, 0)):
            for h in range(2):
                for p in group:
                    if s < 3:
                        kept[s][cell(group, p, at, j, h), row:row + 8, :] = halves[h][p]
                    else:
                        out[out_slot, cell(group, p, 0, j, h)] = halves[h][p]

    def compute(work):
        tasks = [(s, k, j) for s, k in work for j in range(C)]
        fetched = []
        packed = None
        for n, (s, k, j) in enumerate(tasks):
            while len(fetched) < min(n + LOOK + 1, len(tasks)):
                fetched.append(fetch(*tasks[len(fetched)]))
            halves = [collide(fetched[n][h], tau_g, rate36, keep, half_keep) for h in range(2)]
            column = turn(push(halves, lanes), 2 * j)
            packed = column if j == 0 else jnp.where(places >= 2 * j, column, packed)
            keep_plane(s, k, j, halves)
            if j == C - 1:
                if s < 3:
                    zsend[s][lax.rem(k, NS)] = packed
                else:
                    out_z[lax.rem(k, NZ)] = packed
                send(s, k)

    def send(s, k):
        if s < 3:
            for copy in sends(s, lax.rem(k, NS)):
                copy.start()
        else:
            for copy in writes(k, lax.rem(k, 2)) + z_sends(k):
                copy.start()
            face_moves(k, lambda copy, remote: copy.start())

    def arrive(s, k):
        if s == 0:
            load(k, lax.rem(k, 2)).wait()
        else:
            settle(recv_sem.at[s - 1, lax.rem(k + 1, NS)], GROUP_ROWS)

    def reclaim(s, k):
        if s < 3:
            settle(send_sem.at[s, lax.rem(k, NS)], GROUP_ROWS)
        else:
            for copy in writes(k - 2, lax.rem(k, 2)):
                copy.wait()
            face_reclaim(k - 2)

    def stage(s, i):
        k = i - s * LAG
        last = chunks if s < 3 else chunks - 1

        @pl.when((k >= 0) & (k <= last))
        def _():
            if s > 0:
                @pl.when(k == 0)
                def _():
                    arrive(s, -1)
            pl.when(k < chunks + (s == 0))(lambda: arrive(s, k))
            pl.when(k >= (NS if s < 3 else 2))(lambda: reclaim(s, k))
            if s == 0:
                pl.when(k == 0)(lambda: pl.semaphore_wait(barrier, 5))
            if s == 3:
                pl.when(k >= NZ)(lambda: settle(zsend_sem.at[lax.rem(k, NZ)], Z_ROWS))
                pl.when(k >= ZLAG)(lambda: settle(zrecv_sem.at[lax.rem(k - ZLAG, NZ)], Z_ROWS))
            compute([(s, k)])
            if s == 0:
                pl.when(k + 2 <= chunks)(lambda: load(k + 2, lax.rem(k, 2)).start())

    def step(i, carry):
        for s in range(STEPS):
            stage(s, i)
        return carry

    lax.fori_loop(0, chunks + 3 * LAG, step, 0)

    def repeat(low, high, wait):
        def one(n, carry):
            wait(n)
            return carry

        lax.fori_loop(low, high, one, 0)

    for s in range(STEPS - 1):
        repeat(0, NS, lambda slot: settle(send_sem.at[s, slot], GROUP_ROWS))
    repeat(chunks - ZLAG, chunks, lambda k: settle(zrecv_sem.at[lax.rem(k, NZ)], Z_ROWS))
    last = pltpu.make_async_copy(in_z, z_halo, in_sem.at[0])
    last.start()
    repeat(0, NZ, lambda slot: settle(zsend_sem.at[slot], Z_ROWS))
    for k in (chunks - 2, chunks - 1):
        for copy in writes(k, k % 2):
            copy.wait()
        face_reclaim(k)

    def face_arrive(k):
        face_moves(k, lambda copy, remote: copy.wait_recv(), 1)

    repeat(0, PIECES[0] + 1, face_arrive)
    last.wait()


def face_spans(chunks):
    spans = []
    base = 0
    for n, count in enumerate(PIECES):
        high = base + count + 1
        spans.append((n, base, min(high, chunks), base))
        if high > chunks:
            spans.append((n, 0, high - chunks, base - chunks))
        base += count
    return spans


def march(relax_time, body_force, populations):
    nx = populations.shape[1]
    chunks = nx // C
    state = [jax.ShapeDtypeStruct((span(pops, nx),) + TILE, F32) for pops in GROUPS]
    halo_z = (chunks, 3 * TILE[0], TILE[1])
    faces = [
        jax.ShapeDtypeStruct(((count + 1) * span(pops), TILE[1]), F32) for count in PIECES for pops in GROUPS[1:]]
    anywhere = pl.BlockSpec(memory_space=pl.ANY)
    outs = state + [jax.ShapeDtypeStruct(halo_z, F32)] + faces
    dma = pltpu.SemaphoreType.DMA
    stages = STEPS - 1
    wide = 2 * TILE[0]
    return pl.pallas_call(
        functools.partial(march_kernel, chunks),
        out_shape=outs,
        in_specs=[pl.BlockSpec(memory_space=pltpu.SMEM)] * 2 + [anywhere],
        out_specs=[anywhere] * len(outs),
        scratch_shapes=[
            pltpu.VMEM((2, populations.shape[0], C) + populations.shape[2:], F32),
            [
                [ring(GROUPS[0], RP)] * stages, [ring(GROUPS[1], RP, wide)] * stages, [ring(GROUPS[2], RP, wide)] * stages,
                [pltpu.VMEM((NS,) + TILE, F32)] * stages, [pltpu.VMEM((NS,) + halo_z[1:], F32)] * stages,
            ],
            *[pltpu.VMEM((2, span(pops)) + TILE, F32) for pops in GROUPS],
            pltpu.VMEM((NZ,) + TILE, F32), pltpu.VMEM(halo_z, F32),
            dma((2,)), dma((2, 3)), dma((2, 2, 2)), dma((stages, NS)), dma((stages, NS)), dma((NZ,)), dma((NZ,)),
            dma((2, 2)), dma((PIECES[0] + 1, 2)),
            pltpu.VMEM((GROUP_ROWS, TILE[1]), F32),
        ],
        compiler_params=pltpu.CompilerParams(collective_id=0, has_side_effects=True, vmem_limit_bytes=VMEM_BYTES),
        cost_estimate=pl.CostEstimate(flops=10 ** 9, bytes_accessed=10 ** 8, transcendentals=0),
        name="march",
    )(relax_time, body_force, populations)


KW = 3
KR = 4


def final_kernel(
    first, count, aliased, tau_ref, force_ref, g_still, g_up, g_down, halo_up, halo_down, z_in, *rest,
):
    rest = rest[3:] if aliased else rest
    pops, density, velocity, still, up, down, zs, out_f, out_m, in_sem, out_sem, z_sem = rest
    chunks = g_still.shape[0] // span(len(STILL))
    tau = splat(tau_ref[0])
    tau_g = tuple(tau * force_ref[axis] for axis in range(3))
    lanes = lax.broadcasted_iota(jnp.int32, TILE, 1)

    z_copy = pltpu.make_async_copy(z_in, zs, z_sem)
    z_copy.start()

    def loads(t, act):
        slot = lax.rem(t, KR)
        chunk = lax.rem(first + t + chunks - 1, chunks)
        pairs = []
        for pops, state, kept, row in ((GROUPS[0], g_still, still, 0), (5, g_up, up, 8), (5, g_down, down, 0)):
            dst = pl.ds(slot * span(pops), span(pops))
            pairs.append((state.at[pl.ds(chunk * span(pops), span(pops))], kept.at[dst, row:row + 8]))
        src = pl.ds(t * span(5), span(5))
        pairs += [(halo_up.at[src], up.at[dst, 7]), (halo_down.at[src], down.at[dst, 8])]
        for n, (src, dst) in enumerate(pairs):
            act(pltpu.make_async_copy(src, dst, in_sem.at[slot, n]))

    def writes(t):
        slot = lax.rem(t, KW)
        dst = pl.ds(lax.rem(first + t - 1, chunks) * C, C)
        return [
            pltpu.make_async_copy(out_f.at[slot], pops.at[:, dst], out_sem.at[slot, 0]),
            pltpu.make_async_copy(out_m.at[slot, 0], density.at[dst], out_sem.at[slot, 1]),
            pltpu.make_async_copy(out_m.at[slot, pl.ds(1, 3)], velocity.at[:, dst], out_sem.at[slot, 2]),
        ]

    start = lambda copy: copy.start()
    finish = lambda copy: copy.wait()
    for t in range(3):
        loads(t, start)
    loads(0, finish)
    z_copy.wait()

    def step(t, carry):
        @pl.when(t + 2 <= count)
        def _():
            loads(t + 2, start)

        loads(t, finish)

        @pl.when(t > KW)
        def _():
            for copy in writes(t - KW):
                copy.wait()

        slot = lax.rem(t, KW)

        for j in range(C):
            planes = {}
            chunk = {}
            for cx in (1, 0, -1):
                ahead, place = divmod(5 + j - cx, C)
                planes[cx] = (lax.rem(t - 1 + ahead, KR), place)
                chunk[cx] = lax.rem(first - 2 + ahead + t + chunks, chunks)
            zhalo = lambda cx, rows: zs[chunk[cx], rows, :]
            halves = pull(still, up, down, zhalo, planes, lanes)
            for h in range(2):
                f = halves[h]
                rho, u = forced_moments(f, tau_g)
                window = slice(128 * h, 128 * h + 128)
                for p in range(19):
                    out_f[slot, p, j, :, window] = f[p]
                for n, value in enumerate((rho,) + u):
                    out_m[slot, n, j, :, window] = value
        for copy in writes(t):
            copy.start()
        return carry

    lax.fori_loop(1, count + 1, step, 0)
    for t in range(count + 1 - KW, count + 1):
        for copy in writes(t):
            copy.wait()


def final(first, count, relax_time, body_force, state, halos, outs):
    nx = state[0].shape[0] // span(GROUPS[0], 1)
    chunks = nx // C
    anywhere = pl.BlockSpec(memory_space=pl.ANY)
    aliased = outs is not None
    operands = (relax_time, body_force) + state + halos + (outs if aliased else ())
    base = len(operands) - 3
    block = (TILE[0], 2 * TILE[1])
    dma = pltpu.SemaphoreType.DMA
    wide = 2 * TILE[0]
    return pl.pallas_call(
        functools.partial(final_kernel, first, count, aliased),
        out_shape=tuple(jax.ShapeDtypeStruct(lead + (nx,) + block, F32) for lead in ((sum(GROUPS),), (), (3,))),
        in_specs=[pl.BlockSpec(memory_space=pltpu.SMEM)] * 2 + [anywhere] * (len(operands) - 2),
        out_specs=(anywhere,) * 3,
        input_output_aliases={base + n: n for n in range(3)} if aliased else {},
        scratch_shapes=[
            ring(GROUPS[0], KR * C), ring(GROUPS[1], KR * C, wide), ring(GROUPS[2], KR * C, wide),
            pltpu.VMEM((chunks, 3 * TILE[0], TILE[1]), F32),
            pltpu.VMEM((KW, sum(GROUPS), C) + block, F32), pltpu.VMEM((KW, 4, C) + block, F32),
            dma((KR, 5)), dma((KW, 3)), dma,
        ],
        compiler_params=pltpu.CompilerParams(vmem_limit_bytes=VMEM_BYTES if outs is None else VMEM_BYTES * 3 // 4),
        cost_estimate=pl.CostEstimate(flops=count * 10 ** 6, bytes_accessed=count * 3 * 10 ** 6, transcendentals=0),
        name="final",
    )(*operands)


def solution(mesh):
    size_y = mesh.shape["py"]
    size_z = mesh.shape["pz"]
    field_spec = P(None, None, "py", "pz")

    def shift(block, dy, dz):
        pairs = []
        for z in range(size_z):
            for y in range(size_y):
                pairs.append((z * size_y + y, (z + dz) % size_z * size_y + (y + dy) % size_y))
        return lax.ppermute(block, ("pz", "py"), pairs)

    def local_steps(populations, relax_time, body_force):
        tau = relax_time.reshape((1,))
        *state, z_halo = (marched := march(tau, body_force, populations))[:4]
        faces = marched[4:]
        outs = None
        first = 1
        for n, count in enumerate(PIECES):
            up, down = faces[2 * n:2 * n + 2]
            if n:
                up = shift(up, 1, 0)
                down = shift(down, -1, 0)
            outs = final(first, count, tau, body_force, tuple(state), (up, down, z_halo), outs)
            first += count
        return tuple(outs)

    return jax.shard_map(local_steps, mesh=mesh, in_specs=(field_spec, P(), P()), out_specs=(field_spec, P(None, "py", "pz"), field_spec), check_vma=False)
```
